512 devices in a mesh: front: 4 (over x), wide: 16 (over z), narrow: 8 (over y, core).
Axes of the slice: x: 4, y: 4, z: 16, core: 2. Of those that a mesh axis runs over, the one named last changes fastest.
Arguments:
- boundary: int32 [8, 32], P('front'), may hold values from 0 to 63, as said below
- owner: int32 [64], replicated, may hold values from 0 to 7, as said below
- ancestor_cov: bfloat16 [64, 128, 8192], P('narrow', None, 'wide'), may hold values from -1 to 3, as said below
- gain: bfloat16 [8, 4096, 2048], P('front', 'narrow', 'wide'), may hold values from -0.59765625 to 0.59765625
- pivot_inverse: float32 [8, 2048, 256], P('front', 'narrow', 'wide'), may hold values from -6 to 6
Outputs:
- boundary_cov: float32 [8, 2048, 4096], P('front', 'narrow', 'wide')
- diag_cov: float32 [8, 2048, 256], P('front', 'narrow', 'wide')
The draws below stay inside these ranges and needn't reach their ends.
Inputs may be any that keep to these rules, and one draw needn't show every extreme that they name: `boundary`: each row lists 32 distinct ancestor blocks; for every w below 16, positions w * 2 to (w + 1) * 2 - 1 hold blocks from w * 4 to (w + 1) * 4 - 1; for every n below 8, positions n * 4 to (n + 1) * 4 - 1 hold at most 1 block of one owner. In every aligned group of 8 block rows each narrow index owns exactly one; every narrow index owns 8 block rows, and block row r sits in that owner's slot r // 8. `ancestor_cov`: the ancestors' covariance that it holds is symmetric.
All inputs are finite; a program needn't handle non-finite values.
Results may differ from the reference program's by a relative error of at most 0.014.
Values may be sent and summed in bfloat16 or wider, within the bound.
No kernel may reach another device: no remote copies, remote signals or barrier semaphores. Data moves between devices by JAX's collectives and lax.ppermute only.
A program may use at most 64 MiB of HBM per device.

```python
import jax
import jax.numpy as jnp
from jax import lax

BLK = 128
NB = 4096
NP = 2048
IMG = 256
ANC_BLK = 64
FRONTS = 8
NBB = 32
N_WIDE = 16
N_NARROW = 8


def owner_table(key):
    groups = ANC_BLK // N_NARROW
    base_key = jax.random.fold_in(key, 7)

    def one_group(index):
        return jax.random.permutation(jax.random.fold_in(base_key, index), N_NARROW).astype(jnp.int32)
    return jax.vmap(one_group)(jnp.arange(groups, dtype=jnp.int32))


def draw_owner(key, part):
    table = owner_table(key)
    rows = jnp.arange(ANC_BLK, dtype=jnp.int32)
    return table[rows // N_NARROW, rows % N_NARROW].astype(jnp.int32)


def draw_boundary(key, part):
    base_key = jax.random.fold_in(key, 23)
    rows_each = NB // (BLK * N_WIDE)
    range_blocks = ANC_BLK // N_WIDE
    picks_range = range_blocks // rows_each
    classes = (rows_each + N_NARROW - 1) // N_NARROW

    def one_front(member):
        front_key = jax.random.fold_in(base_key, member)
        class_steps = jax.random.randint(jax.random.fold_in(front_key, 1), (N_WIDE, classes), 0, picks_range)
        within = jnp.arange(rows_each, dtype=jnp.int32)[None, :]
        steps_taken = jnp.take(class_steps, jnp.arange(rows_each, dtype=jnp.int32) // N_NARROW, axis=1)
        offsets = within + rows_each * steps_taken
        scores = jax.random.randint(jax.random.fold_in(front_key, 2), (N_WIDE, rows_each), 0, 1 << 20) * rows_each + within
        order = jnp.argsort(scores, axis=1)
        offsets = jnp.take_along_axis(offsets, order, axis=1)
        blocks = offsets + (jnp.arange(N_WIDE, dtype=jnp.int32) * range_blocks)[:, None]
        return blocks.reshape(-1).astype(jnp.int32)
    return jax.vmap(one_front)(jnp.arange(FRONTS, dtype=jnp.int32))


def draw_ancestor_cov(key, part):
    table = owner_table(key)
    full_order = ANC_BLK * BLK
    base_key = jax.random.fold_in(key, 41)
    spread = 0.35 / full_order ** 0.5
    noise = jax.random.normal(jax.random.fold_in(base_key, 1), (full_order, full_order), jnp.float32)
    diagonal = jax.random.uniform(jax.random.fold_in(base_key, 2), (full_order,), jnp.float32, 1.2, 2.0)
    matrix = (noise + jnp.transpose(noise)) * spread
    places = jnp.arange(full_order)
    matrix = matrix.at[places, places].add(diagonal)
    per_owner = ANC_BLK // N_NARROW
    inverse_table = jnp.argsort(table, axis=1).astype(jnp.int32)
    slot_ids = jnp.arange(ANC_BLK, dtype=jnp.int32)
    holder = slot_ids // per_owner
    group = slot_ids % per_owner
    block_row = group * N_NARROW + inverse_table[group, holder]
    return jnp.take(matrix.reshape(ANC_BLK, BLK, full_order), block_row, axis=0).astype(jnp.bfloat16)


def shard_levels(rng, extent, cuts, low, top_value):
    level, own = 1.0, jax.random.fold_in(rng, 6)
    for axis_at, parts in cuts:
        heights = jnp.exp(jax.random.uniform(jax.random.fold_in(own, axis_at), (parts,), jnp.float32, low / len(cuts), top_value / len(cuts)))
        level = level * jnp.repeat(heights, extent[axis_at] // parts).reshape([-1 if axis == axis_at else 1 for axis in range(len(extent))])
    return level


def centred(key, shape, width, most, split=(), kind=jnp.bfloat16):
    factor_of = shard_levels(key, shape, split, -0.22, 0.18) if split else 1.0
    entries = jax.random.normal(key, shape, jnp.float32) * width * factor_of
    return jnp.minimum(jnp.maximum(entries, -most), most).astype(kind)


def setup_inputs(seed: int = 0) -> dict:
    seeds = jax.random.split(jax.random.key(seed), 6)
    return {
        "boundary": draw_boundary(jax.random.fold_in(seeds[5], 71), 0),
        "owner": draw_owner(jax.random.fold_in(seeds[5], 71), 0),
        "ancestor_cov": draw_ancestor_cov(jax.random.fold_in(seeds[5], 71), 0),
        "gain": centred(seeds[3], (FRONTS, NB, NP), 0.08, 0.59765625, ((0, 4), (1, 8), (2, 16))),
        "pivot_inverse": centred(seeds[4], (FRONTS, NP, IMG), 1.0, 6.0, ((0, 4), (1, 8), (2, 16)), jnp.float32),
    }


def front_result(inputs, owner, ancestor_cov):
    boundary_set, gain_panel, pivot_block = inputs
    per_owner = ANC_BLK // N_NARROW
    slot_of = owner * per_owner + jnp.arange(ANC_BLK, dtype=jnp.int32) // N_NARROW
    rows_taken = jnp.take(ancestor_cov, slot_of[boundary_set], axis=0)
    reshaped = rows_taken.reshape(NBB, BLK, ANC_BLK, BLK)
    coupling = jnp.take(reshaped, boundary_set, axis=2).reshape(NB, NB)
    blocks_each = NBB // N_NARROW
    total = jnp.zeros((NB, NP), jnp.float32)
    for narrow in range(N_NARROW):
        start = narrow * blocks_each * BLK
        width_rows = blocks_each * BLK
        partial_value = jnp.dot(lax.dynamic_slice_in_dim(coupling, start, width_rows, 1),
                          lax.dynamic_slice_in_dim(gain_panel, start, width_rows, 0),
                          preferred_element_type=jnp.float32)
        rounded = lax.optimization_barrier(partial_value.astype(jnp.bfloat16))
        total = total + rounded.astype(jnp.float32)
    cross_cov = -jnp.transpose(total)
    cross_low = cross_cov.astype(jnp.bfloat16)
    site_count = NP // IMG
    left_side = cross_low.reshape(site_count, IMG, NB).astype(jnp.float32)
    right_side = gain_panel.reshape(NB, site_count, IMG).astype(jnp.float32)
    blocks_out = jnp.einsum("ipr,riq->ipq", left_side, right_side)
    diag_cov = pivot_block - blocks_out.reshape(NP, IMG)
    return cross_cov, diag_cov


def reference(boundary, owner, ancestor_cov, gain, pivot_inverse):
    def one_front(inputs):
        return front_result(inputs, owner, ancestor_cov)

    boundary_cov, diag_cov = lax.map(one_front, (boundary, gain, pivot_inverse))
    return boundary_cov, diag_cov
```

```python
import jax
import jax.numpy as jnp
from jax import lax
from jax.experimental import pallas as pl
from jax.experimental.pallas import tpu as pltpu
from jax.sharding import Mesh
from jax.sharding import PartitionSpec as P

BLK = 128
NARROW = ("y", "core")
WHOLE = pl.BlockSpec(memory_space=pltpu.VMEM)


def pick_columns(bnd, pos, ancestor):
    def body(bnd_ref, pos_ref, a_ref, o_ref):
        o_ref[...] = a_ref[...]

    slots, rows, _ = ancestor.shape
    fronts = bnd.shape[0]
    return pl.pallas_call(
        body,
        out_shape=jax.ShapeDtypeStruct((slots, fronts, rows, 2 * BLK), ancestor.dtype),
        grid_spec=pltpu.PrefetchScalarGridSpec(
            num_scalar_prefetch=2,
            grid=(fronts, 2),
            in_specs=[
                pl.BlockSpec(
                    (slots, rows, BLK),
                    lambda m, j, b, p: (0, 0, b[m, 2 * p[0] + j] - 4 * p[0]),
                )
            ],
            out_specs=pl.BlockSpec((slots, None, rows, BLK), lambda m, j, b, p: (0, m, 0, j)),
        ),
        name="pick_columns",
    )(bnd, pos, ancestor)


def products(bnd, owner, pos, arrived, chunks):
    fronts, rows, cols = chunks[0].shape
    width = arrived.shape[3]
    blocks = rows // BLK
    count = len(chunks)

    def body(bnd_ref, owner_ref, pos_ref, a_ref, *refs):
        ins, (keep, send) = refs[:count], refs[count:]
        w, n, core = pos_ref[0], pos_ref[1], pos_ref[2]
        for m in range(fronts):
            parts = []
            for j in range(blocks):
                source = owner_ref[bnd_ref[m, blocks * n + j]]
                parts.append(a_ref[source, m].T)
            left = jnp.concatenate(parts, axis=1)
            for r in range(count):
                to = (w + r) & (count - 1)
                slot = 2 * (to >> 2) + (to & 1)
                value = jnp.dot(left, ins[r][m], preferred_element_type=jnp.float32)
                value = value.astype(jnp.bfloat16)
                mine = ((to >> 1) & 1) == core

                @pl.when(mine)
                def _():
                    keep[slot, m] = value

                @pl.when(jnp.logical_not(mine))
                def _():
                    send[slot, m] = value

    shape = jax.ShapeDtypeStruct((count // 2, fronts, width, cols), jnp.bfloat16)
    smem = pl.BlockSpec(memory_space=pltpu.SMEM)
    return pl.pallas_call(
        body,
        out_shape=(shape, shape),
        in_specs=[smem, smem, smem] + [WHOLE] * (1 + count),
        out_specs=(WHOLE, WHOLE),
        name="products",
    )(bnd, owner, pos, arrived, *chunks)


def finish(pos, arrived, g0, g1):
    peers, halves, fronts, rows, cols = arrived.shape

    def body(pos_ref, a_ref, g0_ref, g1_ref, x_ref, d_ref):
        w = pos_ref[0]
        for m in range(fronts):
            lows = []
            for h in range(halves):
                total = a_ref[0, h, m].astype(jnp.float32)
                for s in range(1, peers):
                    total = total + a_ref[s, h, m].astype(jnp.float32)
                cross = -total
                x_ref[m, h * cols : (h + 1) * cols, :] = cross.T
                lows.append(cross.astype(jnp.bfloat16))
            low = jnp.concatenate(lows, axis=1)
            for t, g_ref in enumerate((g0_ref, g1_ref)):
                half = (w + t) & 1
                site = jnp.dot(g_ref[m].T, low, preferred_element_type=jnp.float32)
                d_ref[pl.ds(half * 8, 8), m] = site.astype(jnp.bfloat16).reshape(8, 16, halves * cols)

    return pl.pallas_call(
        body,
        out_shape=(
            jax.ShapeDtypeStruct((fronts, halves * cols, rows), jnp.float32),
            jax.ShapeDtypeStruct((16, fronts, 16, halves * cols), jnp.bfloat16),
        ),
        in_specs=[pl.BlockSpec(memory_space=pltpu.SMEM)] + [WHOLE] * 3,
        out_specs=(WHOLE, WHOLE),
        name="finish",
    )(pos, arrived, g0, g1)


def local(boundary, owner, ancestor_cov, gain, pivot_inverse):
    n_wide = lax.axis_size("wide")
    w = lax.axis_index("wide")
    core = lax.axis_index("core")
    narrow = lax.axis_index("y") * 2 + core
    pos = jnp.stack([w, narrow, core]).astype(jnp.int32)
    fronts = gain.shape[0]

    up = [(i, (i + 1) % n_wide) for i in range(n_wide)]
    down = [(i, (i - 1) % n_wide) for i in range(n_wide)]
    chunks = [None] * n_wide
    chunks[0] = gain
    ahead = behind = gain
    for s in range(1, n_wide // 2 + 1):
        behind = lax.ppermute(behind, "wide", up)
        chunks[n_wide - s] = behind
        if s < n_wide // 2:
            ahead = lax.ppermute(ahead, "wide", down)
            chunks[s] = ahead

    picked = pick_columns(boundary, pos, ancestor_cov)
    arrived = lax.all_to_all(picked, NARROW, split_axis=0, concat_axis=0, tiled=True)

    keep, send = products(boundary, owner, pos, arrived, chunks)
    other = lax.ppermute(send, "core", [(0, 1), (1, 0)])
    pair = (keep.astype(jnp.float32) + other.astype(jnp.float32)).astype(jnp.bfloat16)
    pair = pair.reshape(4, 2, *pair.shape[1:])
    parts = lax.all_to_all(pair, "y", split_axis=0, concat_axis=0, tiled=True)

    late, _ = lax.optimization_barrier((gain, behind))
    rows = gain.shape[1] // 2
    owned = []
    for t in range(2):
        half = (w + t) % 2
        mine = lax.dynamic_slice_in_dim(late, half * rows, rows, 1)
        route = []
        for a in range(n_wide):
            for b in range(8):
                route.append((a * 8 + b, (2 * b + (a + t) % 2) * 8 + a // 2))
        owned.append(lax.ppermute(mine, ("wide", "y", "core"), route))

    boundary_cov, site = finish(pos, parts, *owned)
    sums = lax.all_to_all(site, "wide", split_axis=0, concat_axis=0, tiled=True)
    reduced = jnp.sum(sums.astype(jnp.float32), axis=0)
    diag_cov = pivot_inverse - jnp.swapaxes(reduced, 1, 2)
    return boundary_cov, diag_cov


def solution(mesh):
    fine = Mesh(mesh.devices.reshape(4, 16, 4, 2), ("front", "wide", "y", "core"))
    placed = (
        P("front", None),
        P(),
        P(NARROW, None, "wide"),
        P("front", NARROW, "wide"),
        P("front", NARROW, "wide"),
    )
    return jax.shard_map(
        local,
        mesh=fine,
        in_specs=placed,
        out_specs=(P("front", NARROW, "wide"), P("front", NARROW, "wide")),
        check_vma=False,
    )
```

```python
import jax
import jax.numpy as jnp
from jax import lax
from jax.experimental import pallas as pl
from jax.experimental.pallas import tpu as pltpu
from jax.sharding import Mesh
from jax.sharding import PartitionSpec as P

BLK = 128
NARROW = ("y", "core")
WHOLE = pl.BlockSpec(memory_space=pltpu.VMEM)


def pick_columns(bnd, pos, ancestor):
    def body(bnd_ref, pos_ref, a_ref, o_ref):
        o_ref[...] = a_ref[...]

    slots, rows, _ = ancestor.shape
    fronts = bnd.shape[0]
    return pl.pallas_call(
        body,
        out_shape=jax.ShapeDtypeStruct((slots, fronts, rows, 2 * BLK), ancestor.dtype),
        grid_spec=pltpu.PrefetchScalarGridSpec(
            num_scalar_prefetch=2,
            grid=(fronts, 2),
            in_specs=[
                pl.BlockSpec(
                    (slots, rows, BLK),
                    lambda m, j, b, p: (0, 0, b[m, 2 * p[0] + j] - 4 * p[0]),
                )
            ],
            out_specs=pl.BlockSpec((slots, None, rows, BLK), lambda m, j, b, p: (0, m, 0, j)),
        ),
        name="pick_columns",
    )(bnd, pos, ancestor)


def turned(bnd, owner, pos, own, other):
    _, fronts, rows, width = own.shape
    blocks = bnd.shape[1] // 8

    def body(bnd_ref, owner_ref, pos_ref, own_ref, other_ref, o_ref):
        n = pos_ref[1]
        for m in range(fronts):
            for c, (ref, at) in enumerate(((own_ref, n), (other_ref, n ^ 1))):
                for j in range(blocks):
                    source = owner_ref[bnd_ref[m, blocks * at + j]]
                    first = (c * blocks + j) * rows
                    o_ref[m, :, first : first + rows] = ref[source, m].T

    smem = pl.BlockSpec(memory_space=pltpu.SMEM)
    return pl.pallas_call(
        body,
        out_shape=jax.ShapeDtypeStruct((fronts, width, 2 * blocks * rows), own.dtype),
        in_specs=[smem, smem, smem, WHOLE, WHOLE],
        out_specs=WHOLE,
        name="turned",
    )(bnd, owner, pos, own, other)


def products(left, owns, others):
    fronts, rows, cols = owns[0].shape
    width = left.shape[1]
    count = len(owns)

    def body(left_ref, *refs):
        own, other, out = refs[:count], refs[count : 2 * count], refs[2 * count]
        for m in range(fronts):
            for first in range(0, count, 2):
                group = range(first, min(first + 2, count))
                near = jnp.concatenate([own[s][m] for s in group], axis=1)
                far = jnp.concatenate([other[s][m] for s in group], axis=1)
                value = jnp.dot(left_ref[m, :, :rows], near, preferred_element_type=jnp.float32)
                value += jnp.dot(left_ref[m, :, rows:], far, preferred_element_type=jnp.float32)
                for at, s in enumerate(group):
                    out[s, m] = value[:, at * cols : (at + 1) * cols].astype(jnp.bfloat16)

    flops = 4 * count * fronts * rows * cols * width
    return pl.pallas_call(
        body,
        out_shape=jax.ShapeDtypeStruct((count, fronts, width, cols), jnp.bfloat16),
        in_specs=[WHOLE] * (1 + 2 * count),
        out_specs=WHOLE,
        cost_estimate=pl.CostEstimate(
            flops=flops, transcendentals=0, bytes_accessed=4 * count * fronts * rows * cols * 2
        ),
        name="products",
    )(left, *owns, *others)


def assemble(pos, mine, theirs):
    shape = mine[0].shape[1:]

    def body(pos_ref, *refs):
        out = refs[-1]
        w, core = pos_ref[0], pos_ref[2]
        for from_core, parts in ((core, refs[: len(mine)]), (1 - core, refs[len(mine) : -1])):
            step = 0
            for ref in parts:
                for s in range(ref.shape[0]):
                    to = (w + (2 * from_core - 1) * step) & 15
                    wanted = ((to >> 1) & 1) == core
                    if step == 0:
                        wanted = jnp.logical_and(wanted, from_core == 0)
                    if step == 8:
                        wanted = jnp.logical_and(wanted, from_core == 1)

                    @pl.when(wanted)
                    def _():
                        out[2 * (to >> 2) + (to & 1)] = ref[s]

                    step += 1

    return pl.pallas_call(
        body,
        out_shape=jax.ShapeDtypeStruct((8, *shape), jnp.bfloat16),
        in_specs=[pl.BlockSpec(memory_space=pltpu.SMEM)] + [WHOLE] * (len(mine) + len(theirs)),
        out_specs=WHOLE,
        name="assemble",
    )(pos, *mine, *theirs)


def finish(pos, arrived, pieces):
    peers, halves, fronts, rows, cols = arrived.shape
    count = len(pieces)

    def body(pos_ref, a_ref, *refs):
        gs, (x_ref, d_ref, low_ref) = refs[:count], refs[count:]
        w, n = pos_ref[0], pos_ref[1]
        for m in range(fronts):
            for h in range(halves):
                total = a_ref[0, h, m].astype(jnp.float32)
                for s in range(1, peers):
                    total = total + a_ref[s, h, m].astype(jnp.float32)
                cross = -total
                x_ref[m, h * cols : (h + 1) * cols, :] = cross.T
                low_ref[m, :, h * cols : (h + 1) * cols] = cross.astype(jnp.bfloat16)
        for at, g_ref in enumerate(gs):
            step = at + 1
            down = (w - step % 8) & 15
            up = (w + step) & 15
            first = (down >> 1) == n
            half = jnp.where(first, down & 1, up & 1)

            @pl.when(jnp.logical_or(first, (up >> 1) == n))
            def _():
                for m in range(fronts):
                    site = jnp.dot(g_ref[m].T, low_ref[m], preferred_element_type=jnp.float32)
                    d_ref[pl.ds(half * 8, 8), m] = site.astype(jnp.bfloat16).reshape(8, 16, halves * cols)

    return pl.pallas_call(
        body,
        out_shape=(
            jax.ShapeDtypeStruct((fronts, halves * cols, rows), jnp.float32),
            jax.ShapeDtypeStruct((16, fronts, 16, halves * cols), jnp.bfloat16),
        ),
        in_specs=[pl.BlockSpec(memory_space=pltpu.SMEM)] + [WHOLE] * (1 + count),
        out_specs=(WHOLE, WHOLE),
        scratch_shapes=[pltpu.VMEM((fronts, rows, halves * cols), jnp.bfloat16)],
        name="finish",
    )(pos, arrived, *pieces)


def ring_pairs(cores):
    pairs = []
    for i in range(16):
        if 0 in cores:
            pairs.append((2 * i, 2 * ((i + 1) % 16)))
        if 1 in cores:
            pairs.append((2 * i + 1, 2 * ((i - 1) % 16) + 1))
    return pairs


def piece_pairs(step):
    pairs = []
    for i in range(16):
        down, up = (i - step % 8) % 16, (i + step) % 16
        pairs.append((8 * i + 2 * (i // 4), 8 * i + down // 2))
        pairs.append((8 * i + 2 * (i // 4) + 1, 8 * i + up // 2))
    return pairs


def local(boundary, owner, ancestor_cov, gain, pivot_inverse):
    w = lax.axis_index("wide")
    core = lax.axis_index("core")
    narrow = lax.axis_index("y") * 2 + core
    pos = jnp.stack([w, narrow, core]).astype(jnp.int32)
    swap = [(0, 1), (1, 0)]
    early = 6

    owns, others = [gain], [lax.ppermute(gain, "core", swap)]
    rows = gain.shape[1] // 2
    near = (w >> 1) & 1 == core
    pieces = []
    for step in range(1, 9):
        pairs = ring_pairs((0, 1) if step < 8 else (1,))
        own, other = owns[-1], others[-1]
        if step >= 4:
            own, pieces[step - 4] = lax.optimization_barrier((own, pieces[step - 4]))
        owns.append(lax.ppermute(own, ("wide", "core"), pairs))
        others.append(lax.ppermute(other, ("wide", "core"), pairs))
        a, b = owns[step], others[step]
        if step == 8:
            a = jnp.where(core == 0, owns[0], a)
            b = jnp.where(core == 0, others[0], b)
        held = jnp.where(near, a, b)
        piece = lax.dynamic_slice_in_dim(held, (w & 1) * rows, rows, 1)
        pieces.append(lax.ppermute(piece, ("wide", "y", "core"), piece_pairs(step)))
        if step == 1:
            source, _, _ = lax.optimization_barrier((ancestor_cov, owns[1], others[1]))
            picked = pick_columns(boundary, pos, source)
            arrived = lax.all_to_all(picked, NARROW, split_axis=0, concat_axis=0, tiled=True)
            left = turned(boundary, owner, pos, arrived, lax.ppermute(arrived, "core", swap))

    mine = [products(left, owns[:early], others[:early])]
    theirs = [lax.ppermute(mine[0], "core", swap)]
    mine.append(products(left, owns[early:], others[early:]))
    theirs.append(lax.ppermute(mine[1], "core", swap))
    ready = assemble(pos, mine, theirs)
    ready = ready.reshape(4, 2, *ready.shape[1:])
    parts = lax.all_to_all(ready, "y", split_axis=0, concat_axis=0, tiled=True)

    boundary_cov, site = finish(pos, parts, pieces)
    sums = lax.all_to_all(site, "wide", split_axis=0, concat_axis=0, tiled=True)
    reduced = jnp.sum(sums.astype(jnp.float32), axis=0)
    diag_cov = pivot_inverse - jnp.swapaxes(reduced, 1, 2)
    return boundary_cov, diag_cov


def solution(mesh):
    fine = Mesh(mesh.devices.reshape(4, 16, 4, 2), ("front", "wide", "y", "core"))
    placed = (
        P("front", None),
        P(),
        P(NARROW, None, "wide"),
        P("front", NARROW, "wide"),
        P("front", NARROW, "wide"),
    )
    return jax.shard_map(
        local,
        mesh=fine,
        in_specs=placed,
        out_specs=(P("front", NARROW, "wide"), P("front", NARROW, "wide")),
        check_vma=False,
    )
```

```python
import jax
import jax.numpy as jnp
from jax import lax
from jax.experimental import pallas as pl
from jax.experimental.pallas import tpu as pltpu
from jax.sharding import Mesh
from jax.sharding import PartitionSpec as P

BLK = 128
NARROW = ("y", "core")
WHOLE = pl.BlockSpec(memory_space=pltpu.VMEM)


def pick_columns(bnd, pos, ancestor):
    def body(bnd_ref, pos_ref, a_ref, o_ref):
        o_ref[...] = a_ref[...]

    slots, rows, _ = ancestor.shape
    fronts = bnd.shape[0]
    return pl.pallas_call(
        body,
        out_shape=jax.ShapeDtypeStruct((slots, fronts, rows, 2 * BLK), ancestor.dtype),
        grid_spec=pltpu.PrefetchScalarGridSpec(
            num_scalar_prefetch=2,
            grid=(fronts, 2),
            in_specs=[
                pl.BlockSpec(
                    (slots, rows, BLK),
                    lambda m, j, b, p: (0, 0, b[m, 2 * p[0] + j] - 4 * p[0]),
                )
            ],
            out_specs=pl.BlockSpec((slots, None, rows, BLK), lambda m, j, b, p: (0, m, 0, j)),
        ),
        name="pick_columns",
    )(bnd, pos, ancestor)


def turned(bnd, owner, pos, own, other):
    _, fronts, rows, width = own.shape
    blocks = bnd.shape[1] // 8

    def body(bnd_ref, owner_ref, pos_ref, own_ref, other_ref, o_ref):
        n = pos_ref[1]
        for m in range(fronts):
            for c, (ref, at) in enumerate(((own_ref, n), (other_ref, n ^ 1))):
                for j in range(blocks):
                    source = owner_ref[bnd_ref[m, blocks * at + j]]
                    first = (c * blocks + j) * rows
                    o_ref[m, :, first : first + rows] = ref[source, m].T

    smem = pl.BlockSpec(memory_space=pltpu.SMEM)
    return pl.pallas_call(
        body,
        out_shape=jax.ShapeDtypeStruct((fronts, width, 2 * blocks * rows), own.dtype),
        in_specs=[smem, smem, smem, WHOLE, WHOLE],
        out_specs=WHOLE,
        name="turned",
    )(bnd, owner, pos, own, other)


def products(left, owns, others):
    fronts, rows, cols = owns[0].shape
    width = left.shape[1]
    count = len(owns)

    def body(left_ref, *refs):
        own, other, out = refs[:count], refs[count : 2 * count], refs[2 * count]
        for m in range(fronts):
            for first in range(0, count, 2):
                group = range(first, min(first + 2, count))
                near = jnp.concatenate([own[s][m] for s in group], axis=1)
                far = jnp.concatenate([other[s][m] for s in group], axis=1)
                value = jnp.dot(left_ref[m, :, :rows], near, preferred_element_type=jnp.float32)
                value += jnp.dot(left_ref[m, :, rows:], far, preferred_element_type=jnp.float32)
                for at, s in enumerate(group):
                    out[s, m] = value[:, at * cols : (at + 1) * cols].astype(jnp.bfloat16)

    flops = 4 * count * fronts * rows * cols * width
    return pl.pallas_call(
        body,
        out_shape=jax.ShapeDtypeStruct((count, fronts, width, cols), jnp.bfloat16),
        in_specs=[WHOLE] * (1 + 2 * count),
        out_specs=WHOLE,
        cost_estimate=pl.CostEstimate(
            flops=flops, transcendentals=0, bytes_accessed=4 * count * fronts * rows * cols * 2
        ),
        name="products",
    )(left, *owns, *others)


def assemble(pos, mine, theirs):
    shape = mine[0].shape[1:]

    def body(pos_ref, *refs):
        out = refs[-1]
        w, core = pos_ref[0], pos_ref[2]
        for from_core, parts in ((core, refs[: len(mine)]), (1 - core, refs[len(mine) : -1])):
            step = 0
            for ref in parts:
                for s in range(ref.shape[0]):
                    to = (w + (2 * from_core - 1) * step) & 15
                    wanted = ((to >> 1) & 1) == core
                    if step == 0:
                        wanted = jnp.logical_and(wanted, from_core == 0)
                    if step == 8:
                        wanted = jnp.logical_and(wanted, from_core == 1)

                    @pl.when(wanted)
                    def _():
                        out[2 * (to >> 2) + (to & 1)] = ref[s]

                    step += 1

    return pl.pallas_call(
        body,
        out_shape=jax.ShapeDtypeStruct((8, *shape), jnp.bfloat16),
        in_specs=[pl.BlockSpec(memory_space=pltpu.SMEM)] + [WHOLE] * (len(mine) + len(theirs)),
        out_specs=WHOLE,
        name="assemble",
    )(pos, *mine, *theirs)


def finish(pos, arrived, pieces):
    peers, halves, fronts, rows, cols = arrived.shape
    count = len(pieces)

    def body(pos_ref, a_ref, *refs):
        gs, (x_ref, d_ref, low_ref) = refs[:count], refs[count:]
        w, n = pos_ref[0], pos_ref[1]
        for m in range(fronts):
            for h in range(halves):
                total = a_ref[0, h, m].astype(jnp.float32)
                for s in range(1, peers):
                    total = total + a_ref[s, h, m].astype(jnp.float32)
                cross = -total
                x_ref[m, h * cols : (h + 1) * cols, :] = cross.T
                low_ref[m, :, h * cols : (h + 1) * cols] = cross.astype(jnp.bfloat16)
        for at, g_ref in enumerate(gs):
            step = at + 1
            down = (w - step % 8) & 15
            up = (w + step) & 15
            first = (down >> 1) == n
            half = jnp.where(first, down & 1, up & 1)

            @pl.when(jnp.logical_or(first, (up >> 1) == n))
            def _():
                for m in range(fronts):
                    site = jnp.dot(g_ref[m].T, low_ref[m], preferred_element_type=jnp.float32)
                    d_ref[pl.ds(half * 8, 8), m] = site.astype(jnp.bfloat16).reshape(8, 16, halves * cols)

    return pl.pallas_call(
        body,
        out_shape=(
            jax.ShapeDtypeStruct((fronts, halves * cols, rows), jnp.float32),
            jax.ShapeDtypeStruct((16, fronts, 16, halves * cols), jnp.bfloat16),
        ),
        in_specs=[pl.BlockSpec(memory_space=pltpu.SMEM)] + [WHOLE] * (1 + count),
        out_specs=(WHOLE, WHOLE),
        scratch_shapes=[pltpu.VMEM((fronts, rows, halves * cols), jnp.bfloat16)],
        name="finish",
    )(pos, arrived, *pieces)


def ring_pairs(cores):
    pairs = []
    for i in range(16):
        if 0 in cores:
            pairs.append((2 * i, 2 * ((i + 1) % 16)))
        if 1 in cores:
            pairs.append((2 * i + 1, 2 * ((i - 1) % 16) + 1))
    return pairs


def piece_pairs(step):
    pairs = []
    for i in range(16):
        down, up = (i - step % 8) % 16, (i + step) % 16
        pairs.append((8 * i + 2 * (i // 4), 8 * i + down // 2))
        pairs.append((8 * i + 2 * (i // 4) + 1, 8 * i + up // 2))
    return pairs


def level(boundary, owner, ancestor_cov, gain, pivot_inverse):
    w = lax.axis_index("wide")
    core = lax.axis_index("core")
    narrow = lax.axis_index("y") * 2 + core
    pos = jnp.stack([w, narrow, core]).astype(jnp.int32)
    swap = [(0, 1), (1, 0)]
    early = 6

    owns = [gain]
    others = [lax.ppermute(gain, "core", swap)]
    rows = gain.shape[1] // 2
    near = (w >> 1) & 1 == core
    pieces = []
    for step in range(1, 9):
        pairs = ring_pairs((0, 1) if step < 8 else (1,))
        owns.append(lax.ppermute(owns[-1], ("wide", "core"), pairs))
        others.append(lax.ppermute(others[-1], ("wide", "core"), pairs))
        a, b = owns[step], others[step]
        if step == 8:
            a = jnp.where(core == 0, owns[0], a)
            b = jnp.where(core == 0, others[0], b)
        held = jnp.where(near, a, b)
        piece = lax.dynamic_slice_in_dim(held, (w & 1) * rows, rows, 1)
        pieces.append(lax.ppermute(piece, ("wide", "y", "core"), piece_pairs(step)))
        if step == 1:
            picked = pick_columns(boundary, pos, ancestor_cov)
            arrived = lax.all_to_all(picked, NARROW, split_axis=0, concat_axis=0, tiled=True)
            paired = lax.ppermute(arrived, "core", swap)
            left = turned(boundary, owner, pos, arrived, paired)

    mine = [products(left, owns[:early], others[:early])]
    theirs = [lax.ppermute(mine[0], "core", swap)]
    mine.append(products(left, owns[early:], others[early:]))
    theirs.append(lax.ppermute(mine[1], "core", swap))
    ready = assemble(pos, mine, theirs)
    ready = ready.reshape(4, 2, *ready.shape[1:])
    parts = lax.all_to_all(ready, "y", split_axis=0, concat_axis=0, tiled=True)

    boundary_cov, site = finish(pos, parts, pieces)
    sums = lax.all_to_all(site, "wide", split_axis=0, concat_axis=0, tiled=True)
    reduced = jnp.sum(sums.astype(jnp.float32), axis=0)
    diag_cov = pivot_inverse - jnp.swapaxes(reduced, 1, 2)
    return boundary_cov, diag_cov


def solution(mesh):
    fine = Mesh(mesh.devices.reshape(4, 16, 4, 2), ("front", "wide", "y", "core"))
    placed = (
        P("front", None),
        P(),
        P(NARROW, None, "wide"),
        P("front", NARROW, "wide"),
        P("front", NARROW, "wide"),
    )
    return jax.shard_map(
        level,
        mesh=fine,
        in_specs=placed,
        out_specs=(P("front", NARROW, "wide"), P("front", NARROW, "wide")),
        check_vma=False,
    )
```

```python
import jax
import jax.numpy as jnp
from jax import lax
from jax.experimental import pallas as pl
from jax.experimental.pallas import tpu as pltpu
from jax.sharding import Mesh
from jax.sharding import PartitionSpec as P

BLK = 128
NARROW = ("y", "core")
WHOLE = pl.BlockSpec(memory_space=pltpu.VMEM)


def turned(bnd, owner, pos, own, other):
    fronts, rows = bnd.shape[0], own.shape[1]
    blocks, width = bnd.shape[1] // 8, 2 * BLK

    def body(bnd_ref, owner_ref, pos_ref, own_ref, other_ref, o_ref):
        w, n = pos_ref[0], pos_ref[1]
        for m in range(fronts):
            columns = [
                pl.ds(pl.multiple_of((bnd_ref[m, 2 * w + b] - 4 * w) * BLK, BLK), BLK) for b in range(2)
            ]
            for c, (ref, at) in enumerate(((own_ref, n), (other_ref, n ^ 1))):
                for j in range(blocks):
                    source = owner_ref[bnd_ref[m, blocks * at + j]]
                    first = (c * blocks + j) * rows
                    for b in range(2):
                        block = ref[source, :, columns[b]]
                        o_ref[m, b * BLK : (b + 1) * BLK, first : first + rows] = block.T

    smem = pl.BlockSpec(memory_space=pltpu.SMEM)
    return pl.pallas_call(
        body,
        out_shape=jax.ShapeDtypeStruct((fronts, width, 2 * blocks * rows), own.dtype),
        in_specs=[smem, smem, smem, WHOLE, WHOLE],
        out_specs=WHOLE,
        name="turned",
    )(bnd, owner, pos, own, other)


def products(left, owns, others):
    fronts, rows, cols = owns[0].shape
    width = left.shape[1]
    count = len(owns)

    def body(left_ref, *refs):
        own, other, out = refs[:count], refs[count : 2 * count], refs[2 * count]
        for m in range(fronts):
            for first in range(0, count, 2):
                group = range(first, min(first + 2, count))
                near = jnp.concatenate([own[s][m] for s in group], axis=1)
                far = jnp.concatenate([other[s][m] for s in group], axis=1)
                value = jnp.dot(left_ref[m, :, :rows], near, preferred_element_type=jnp.float32)
                value += jnp.dot(left_ref[m, :, rows:], far, preferred_element_type=jnp.float32)
                for at, s in enumerate(group):
                    out[s, m] = value[:, at * cols : (at + 1) * cols].astype(jnp.bfloat16)

    flops = 4 * count * fronts * rows * cols * width
    return pl.pallas_call(
        body,
        out_shape=jax.ShapeDtypeStruct((count, fronts, width, cols), jnp.bfloat16),
        in_specs=[WHOLE] * (1 + 2 * count),
        out_specs=WHOLE,
        cost_estimate=pl.CostEstimate(
            flops=flops, transcendentals=0, bytes_accessed=4 * count * fronts * rows * cols * 2
        ),
        name="products",
    )(left, *owns, *others)


def assemble(pos, mine, theirs):
    shape = mine[0].shape[1:]

    def body(pos_ref, *refs):
        out = refs[-1]
        w, core = pos_ref[0], pos_ref[2]
        for from_core, parts in ((core, refs[: len(mine)]), (1 - core, refs[len(mine) : -1])):
            step = 0
            for ref in parts:
                for s in range(ref.shape[0]):
                    to = (w + (2 * from_core - 1) * step) & 15
                    wanted = ((to >> 1) & 1) == core
                    if step == 0:
                        wanted = jnp.logical_and(wanted, from_core == 0)
                    if step == 8:
                        wanted = jnp.logical_and(wanted, from_core == 1)

                    @pl.when(wanted)
                    def _():
                        out[2 * (to >> 2) + (to & 1)] = ref[s]

                    step += 1

    return pl.pallas_call(
        body,
        out_shape=jax.ShapeDtypeStruct((8, *shape), jnp.bfloat16),
        in_specs=[pl.BlockSpec(memory_space=pltpu.SMEM)] + [WHOLE] * (len(mine) + len(theirs)),
        out_specs=WHOLE,
        name="assemble",
    )(pos, *mine, *theirs)


def finish(pos, arrived, pieces):
    peers, halves, fronts, rows, cols = arrived.shape
    count = len(pieces)

    def body(pos_ref, a_ref, *refs):
        gs, (x_ref, d_ref, low_ref) = refs[:count], refs[count:]
        w, n = pos_ref[0], pos_ref[1]
        for m in range(fronts):
            for h in range(halves):
                total = a_ref[0, h, m].astype(jnp.float32)
                for s in range(1, peers):
                    total = total + a_ref[s, h, m].astype(jnp.float32)
                cross = -total
                x_ref[m, h * cols : (h + 1) * cols, :] = cross.T
                low_ref[m, :, h * cols : (h + 1) * cols] = cross.astype(jnp.bfloat16)
        for at, g_ref in enumerate(gs):
            step = at + 1
            down = (w - step % 8) & 15
            up = (w + step) & 15
            first = (down >> 1) == n
            half = jnp.where(first, down & 1, up & 1)

            @pl.when(jnp.logical_or(first, (up >> 1) == n))
            def _():
                for m in range(fronts):
                    site = jnp.dot(g_ref[m].T, low_ref[m], preferred_element_type=jnp.float32)
                    d_ref[pl.ds(half * 8, 8), m] = site.astype(jnp.bfloat16).reshape(8, 16, halves * cols)

    return pl.pallas_call(
        body,
        out_shape=(
            jax.ShapeDtypeStruct((fronts, halves * cols, rows), jnp.float32),
            jax.ShapeDtypeStruct((16, fronts, 16, halves * cols), jnp.bfloat16),
        ),
        in_specs=[pl.BlockSpec(memory_space=pltpu.SMEM)] + [WHOLE] * (1 + count),
        out_specs=(WHOLE, WHOLE),
        scratch_shapes=[pltpu.VMEM((fronts, rows, halves * cols), jnp.bfloat16)],
        name="finish",
    )(pos, arrived, *pieces)


def ring_pairs(cores):
    pairs = []
    for i in range(16):
        if 0 in cores:
            pairs.append((2 * i, 2 * ((i + 1) % 16)))
        if 1 in cores:
            pairs.append((2 * i + 1, 2 * ((i - 1) % 16) + 1))
    return pairs


def piece_pairs(step):
    pairs = []
    for i in range(16):
        down, up = (i - step % 8) % 16, (i + step) % 16
        pairs.append((8 * i + 2 * (i // 4), 8 * i + down // 2))
        pairs.append((8 * i + 2 * (i // 4) + 1, 8 * i + up // 2))
    return pairs


def level(boundary, owner, ancestor_cov, gain, pivot_inverse):
    w = lax.axis_index("wide")
    core = lax.axis_index("core")
    narrow = lax.axis_index("y") * 2 + core
    pos = jnp.stack([w, narrow, core]).astype(jnp.int32)
    swap = [(0, 1), (1, 0)]
    early = 7

    owns = [gain]
    others = [lax.ppermute(gain, "core", swap)]
    rows = gain.shape[1] // 2
    near = (w >> 1) & 1 == core
    pieces = []
    for step in range(1, 9):
        pairs = ring_pairs((0, 1) if step < 8 else (1,))
        owns.append(lax.ppermute(owns[-1], ("wide", "core"), pairs))
        others.append(lax.ppermute(others[-1], ("wide", "core"), pairs))
        a, b = owns[step], others[step]
        if step == 8:
            a = jnp.where(core == 0, owns[0], a)
            b = jnp.where(core == 0, others[0], b)
        held = jnp.where(near, a, b)
        piece = lax.dynamic_slice_in_dim(held, (w & 1) * rows, rows, 1)
        pieces.append(lax.ppermute(piece, ("wide", "y", "core"), piece_pairs(step)))
        if step == 1:
            arrived = lax.all_to_all(ancestor_cov, NARROW, split_axis=0, concat_axis=0, tiled=True)
            paired = lax.ppermute(arrived, "core", swap)
            left = turned(boundary, owner, pos, arrived, paired)

    mine = [products(left, owns[:early], others[:early])]
    theirs = [lax.ppermute(mine[0], "core", swap)]
    mine.append(products(left, owns[early:], others[early:]))
    theirs.append(lax.ppermute(mine[1], "core", swap))
    ready = assemble(pos, mine, theirs)
    ready = ready.reshape(4, 2, *ready.shape[1:])
    parts = lax.all_to_all(ready, "y", split_axis=0, concat_axis=0, tiled=True)

    boundary_cov, site = finish(pos, parts, pieces)
    sums = lax.all_to_all(site, "wide", split_axis=0, concat_axis=0, tiled=True)
    reduced = jnp.sum(sums.astype(jnp.float32), axis=0)
    diag_cov = pivot_inverse - jnp.swapaxes(reduced, 1, 2)
    return boundary_cov, diag_cov


def solution(mesh):
    fine = Mesh(mesh.devices.reshape(4, 16, 4, 2), ("front", "wide", "y", "core"))
    placed = (
        P("front", None),
        P(),
        P(NARROW, None, "wide"),
        P("front", NARROW, "wide"),
        P("front", NARROW, "wide"),
    )
    return jax.shard_map(
        level,
        mesh=fine,
        in_specs=placed,
        out_specs=(P("front", NARROW, "wide"), P("front", NARROW, "wide")),
        check_vma=False,
    )
```

```python
import jax
import jax.numpy as jnp
from jax import lax
from jax.experimental import pallas as pl
from jax.experimental.pallas import tpu as pltpu
from jax.sharding import Mesh
from jax.sharding import PartitionSpec as P

BLK = 128
NARROW = ("y", "core")
WHOLE = pl.BlockSpec(memory_space=pltpu.VMEM)


def turned(bnd, owner, pos, own, other):
    fronts, rows = bnd.shape[0], own.shape[1]
    blocks, width = bnd.shape[1] // 8, 2 * BLK

    def body(bnd_ref, owner_ref, pos_ref, own_ref, other_ref, o_ref):
        w, n = pos_ref[0], pos_ref[1]
        for m in range(fronts):
            columns = [
                pl.ds(pl.multiple_of((bnd_ref[m, 2 * w + b] - 4 * w) * BLK, BLK), BLK) for b in range(2)
            ]
            for c, (ref, at) in enumerate(((own_ref, n), (other_ref, n ^ 1))):
                for j in range(blocks):
                    source = owner_ref[bnd_ref[m, blocks * at + j]]
                    first = (c * blocks + j) * rows
                    for b in range(2):
                        block = ref[source, :, columns[b]]
                        o_ref[m, b * BLK : (b + 1) * BLK, first : first + rows] = block.T

    smem = pl.BlockSpec(memory_space=pltpu.SMEM)
    return pl.pallas_call(
        body,
        out_shape=jax.ShapeDtypeStruct((fronts, width, 2 * blocks * rows), own.dtype),
        in_specs=[smem, smem, smem, WHOLE, WHOLE],
        out_specs=WHOLE,
        name="turned",
    )(bnd, owner, pos, own, other)


def products(left, owns, others):
    fronts, rows, cols = owns[0].shape
    width = left.shape[1]
    count = len(owns)

    def body(left_ref, *refs):
        own, other, out = refs[:count], refs[count : 2 * count], refs[2 * count]
        for m in range(fronts):
            for first in range(0, count, 2):
                group = range(first, min(first + 2, count))
                near = jnp.concatenate([own[s][m] for s in group], axis=1)
                far = jnp.concatenate([other[s][m] for s in group], axis=1)
                value = jnp.dot(left_ref[m, :, :rows], near, preferred_element_type=jnp.float32)
                value += jnp.dot(left_ref[m, :, rows:], far, preferred_element_type=jnp.float32)
                for at, s in enumerate(group):
                    out[s, m] = value[:, at * cols : (at + 1) * cols].astype(jnp.bfloat16)

    flops = 4 * count * fronts * rows * cols * width
    return pl.pallas_call(
        body,
        out_shape=jax.ShapeDtypeStruct((count, fronts, width, cols), jnp.bfloat16),
        in_specs=[WHOLE] * (1 + 2 * count),
        out_specs=WHOLE,
        cost_estimate=pl.CostEstimate(
            flops=flops, transcendentals=0, bytes_accessed=4 * count * fronts * rows * cols * 2
        ),
        name="products",
    )(left, *owns, *others)


def assemble(pos, mine, theirs):
    shape = mine[0].shape[1:]

    def body(pos_ref, *refs):
        out = refs[-1]
        w, core = pos_ref[0], pos_ref[2]
        for from_core, parts in ((core, refs[: len(mine)]), (1 - core, refs[len(mine) : -1])):
            step = 0
            for ref in parts:
                for s in range(ref.shape[0]):
                    to = (w + (2 * from_core - 1) * step) & 15
                    wanted = ((to >> 1) & 1) == core
                    if step == 0:
                        wanted = jnp.logical_and(wanted, from_core == 0)
                    if step == 8:
                        wanted = jnp.logical_and(wanted, from_core == 1)

                    @pl.when(wanted)
                    def _():
                        out[2 * (to >> 2) + (to & 1)] = ref[s]

                    step += 1

    return pl.pallas_call(
        body,
        out_shape=jax.ShapeDtypeStruct((8, *shape), jnp.bfloat16),
        in_specs=[pl.BlockSpec(memory_space=pltpu.SMEM)] + [WHOLE] * (len(mine) + len(theirs)),
        out_specs=WHOLE,
        name="assemble",
    )(pos, *mine, *theirs)


def finish(pos, arrived, pieces):
    peers, halves, fronts, rows, cols = arrived.shape

    def body(pos_ref, a_ref, g_ref, x_ref, d_ref):
        w = pos_ref[0]
        for m in range(fronts):
            lows = []
            for h in range(halves):
                total = a_ref[0, h, m].astype(jnp.float32)
                for s in range(1, peers):
                    total = total + a_ref[s, h, m].astype(jnp.float32)
                cross = -total
                x_ref[m, h * cols : (h + 1) * cols, :] = cross.T
                lows.append(cross.astype(jnp.bfloat16))
            low = jnp.concatenate(lows, axis=1)
            for t in range(2):
                half = (w + t) & 1
                site = jnp.dot(g_ref[t, m].T, low, preferred_element_type=jnp.float32)
                d_ref[pl.ds(half * 8, 8), m] = site.astype(jnp.bfloat16).reshape(8, 16, halves * cols)

    return pl.pallas_call(
        body,
        out_shape=(
            jax.ShapeDtypeStruct((fronts, halves * cols, rows), jnp.float32),
            jax.ShapeDtypeStruct((16, fronts, 16, halves * cols), jnp.bfloat16),
        ),
        in_specs=[pl.BlockSpec(memory_space=pltpu.SMEM)] + [WHOLE] * 2,
        out_specs=(WHOLE, WHOLE),
        name="finish",
    )(pos, arrived, pieces)


def ring_pairs(cores):
    pairs = []
    for i in range(16):
        if 0 in cores:
            pairs.append((2 * i, 2 * ((i + 1) % 16)))
        if 1 in cores:
            pairs.append((2 * i + 1, 2 * ((i - 1) % 16) + 1))
    return pairs


def turn_pairs(way):
    return [(4 * i + y, 4 * i + (y + way * (i // 4)) % 4) for i in range(16) for y in range(4)]


def block_pairs(t):
    pairs = []
    for i in range(16):
        for y in range(4):
            for c in range(2):
                to = 4 * ((y - i // 4) % 4) + 2 * c + (i + t) % 2
                pairs.append((8 * i + 2 * y + c, 8 * to + 2 * y + (i // 2) % 2))
    return pairs


def level(boundary, owner, ancestor_cov, gain, pivot_inverse):
    w = lax.axis_index("wide")
    core = lax.axis_index("core")
    narrow = lax.axis_index("y") * 2 + core
    pos = jnp.stack([w, narrow, core]).astype(jnp.int32)
    swap = [(0, 1), (1, 0)]
    early = 7

    owns = [gain]
    others = [lax.ppermute(gain, "core", swap)]
    rows = gain.shape[1] // 2
    turned_gain = lax.ppermute(gain, ("wide", "y"), turn_pairs(1))
    blocks = []
    for t in range(2):
        half = lax.dynamic_slice_in_dim(turned_gain, ((w + t) & 1) * rows, rows, 1)
        blocks.append(lax.ppermute(half, ("wide", "y", "core"), block_pairs(t)))
    blocks = jnp.stack(blocks)
    pieces = lax.ppermute(blocks, ("wide", "y"), turn_pairs(-1))
    for step in range(1, 9):
        pairs = ring_pairs((0, 1) if step < 8 else (1,))
        owns.append(lax.ppermute(owns[-1], ("wide", "core"), pairs))
        others.append(lax.ppermute(others[-1], ("wide", "core"), pairs))
        if step == 1:
            arrived = lax.all_to_all(ancestor_cov, NARROW, split_axis=0, concat_axis=0, tiled=True)
            paired = lax.ppermute(arrived, "core", swap)
            left = turned(boundary, owner, pos, arrived, paired)

    mine = [products(left, owns[:early], others[:early])]
    theirs = [lax.ppermute(mine[0], "core", swap)]
    mine.append(products(left, owns[early:], others[early:]))
    theirs.append(lax.ppermute(mine[1], "core", swap))
    ready = assemble(pos, mine, theirs)
    ready = ready.reshape(4, 2, *ready.shape[1:])
    parts = lax.all_to_all(ready, "y", split_axis=0, concat_axis=0, tiled=True)

    boundary_cov, site = finish(pos, parts, pieces)
    sums = lax.all_to_all(site, "wide", split_axis=0, concat_axis=0, tiled=True)
    reduced = jnp.sum(sums.astype(jnp.float32), axis=0)
    diag_cov = pivot_inverse - jnp.swapaxes(reduced, 1, 2)
    return boundary_cov, diag_cov


def solution(mesh):
    fine = Mesh(mesh.devices.reshape(4, 16, 4, 2), ("front", "wide", "y", "core"))
    placed = (
        P("front", None),
        P(),
        P(NARROW, None, "wide"),
        P("front", NARROW, "wide"),
        P("front", NARROW, "wide"),
    )
    return jax.shard_map(
        level,
        mesh=fine,
        in_specs=placed,
        out_specs=(P("front", NARROW, "wide"), P("front", NARROW, "wide")),
        check_vma=False,
    )
```

```python
import jax
import jax.numpy as jnp
from jax import lax
from jax.experimental import pallas as pl
from jax.experimental.pallas import tpu as pltpu
from jax.sharding import Mesh
from jax.sharding import PartitionSpec as P

BLK = 128
NARROW = ("y", "core")
WIDE = ("block", "place")
WHOLE = pl.BlockSpec(memory_space=pltpu.VMEM)


def turned(bnd, owner, pos, own, other):
    fronts, rows = bnd.shape[0], own.shape[1]
    blocks, width = bnd.shape[1] // 8, 2 * BLK

    def body(bnd_ref, owner_ref, pos_ref, own_ref, other_ref, o_ref):
        w, n = pos_ref[0], pos_ref[1]
        for m in range(fronts):
            columns = [
                pl.ds(pl.multiple_of((bnd_ref[m, 2 * w + b] - 4 * w) * BLK, BLK), BLK) for b in range(2)
            ]
            for c, (ref, at) in enumerate(((own_ref, n), (other_ref, n ^ 1))):
                for j in range(blocks):
                    source = owner_ref[bnd_ref[m, blocks * at + j]]
                    first = (c * blocks + j) * rows
                    for b in range(2):
                        block = ref[source, :, columns[b]]
                        o_ref[m, b * BLK : (b + 1) * BLK, first : first + rows] = block.T

    smem = pl.BlockSpec(memory_space=pltpu.SMEM)
    return pl.pallas_call(
        body,
        out_shape=jax.ShapeDtypeStruct((fronts, width, 2 * blocks * rows), own.dtype),
        in_specs=[smem, smem, smem, WHOLE, WHOLE],
        out_specs=WHOLE,
        name="turned",
    )(bnd, owner, pos, own, other)


def products(left, owns, others):
    fronts, rows, cols = owns[0].shape
    width = left.shape[1]
    count = len(owns)

    def body(left_ref, *refs):
        own, other, out = refs[:count], refs[count : 2 * count], refs[2 * count]
        for m in range(fronts):
            for first in range(0, count, 2):
                group = range(first, min(first + 2, count))
                near = jnp.concatenate([own[s][m] for s in group], axis=1)
                far = jnp.concatenate([other[s][m] for s in group], axis=1)
                value = jnp.dot(left_ref[m, :, :rows], near, preferred_element_type=jnp.float32)
                value += jnp.dot(left_ref[m, :, rows:], far, preferred_element_type=jnp.float32)
                for at, s in enumerate(group):
                    out[s, m] = value[:, at * cols : (at + 1) * cols].astype(jnp.bfloat16)

    flops = 4 * count * fronts * rows * cols * width
    return pl.pallas_call(
        body,
        out_shape=jax.ShapeDtypeStruct((count, fronts, width, cols), jnp.bfloat16),
        in_specs=[WHOLE] * (1 + 2 * count),
        out_specs=WHOLE,
        cost_estimate=pl.CostEstimate(
            flops=flops, transcendentals=0, bytes_accessed=4 * count * fronts * rows * cols * 2
        ),
        name="products",
    )(left, *owns, *others)


def assemble(pos, mine, theirs):
    shape = mine[0].shape[1:]

    def body(pos_ref, *refs):
        out = refs[-1]
        w, core = pos_ref[0], pos_ref[2]
        for from_core, parts in ((core, refs[: len(mine)]), (1 - core, refs[len(mine) : -1])):
            step = 0
            for ref in parts:
                for s in range(ref.shape[0]):
                    to = (w + (2 * from_core - 1) * step) & 15
                    wanted = ((to >> 1) & 1) == core
                    if step == 0:
                        wanted = jnp.logical_and(wanted, from_core == 0)
                    if step == 8:
                        wanted = jnp.logical_and(wanted, from_core == 1)

                    @pl.when(wanted)
                    def _():
                        out[2 * (to >> 2) + (to & 1)] = ref[s]

                    step += 1

    return pl.pallas_call(
        body,
        out_shape=jax.ShapeDtypeStruct((8, *shape), jnp.bfloat16),
        in_specs=[pl.BlockSpec(memory_space=pltpu.SMEM)] + [WHOLE] * (len(mine) + len(theirs)),
        out_specs=WHOLE,
        name="assemble",
    )(pos, *mine, *theirs)


def finish(pos, arrived, pieces):
    peers, halves, fronts, rows, cols = arrived.shape
    count = len(pieces)

    def body(pos_ref, a_ref, *refs):
        gs, (x_ref, d_ref, low_ref) = refs[:count], refs[count:]
        w, n = pos_ref[0], pos_ref[1]
        for m in range(fronts):
            for h in range(halves):
                total = a_ref[0, h, m].astype(jnp.float32)
                for s in range(1, peers):
                    total = total + a_ref[s, h, m].astype(jnp.float32)
                cross = -total
                x_ref[m, h * cols : (h + 1) * cols, :] = cross.T
                low_ref[m, :, h * cols : (h + 1) * cols] = cross.astype(jnp.bfloat16)
        for at, g_ref in enumerate(gs):
            step = at + 1
            down = (w - step % 8) & 15
            up = (w + step) & 15
            first = (down >> 1) == n
            half = jnp.where(first, down & 1, up & 1)

            @pl.when(jnp.logical_or(first, (up >> 1) == n))
            def _():
                for m in range(fronts):
                    site = jnp.dot(g_ref[m].T, low_ref[m], preferred_element_type=jnp.float32)
                    site = site.astype(jnp.bfloat16).reshape(2, 4, 16, halves * cols)
                    for block in range(2):
                        for place in range(4):
                            d_ref[place, 2 * half + block, m] = site[block, place]

    return pl.pallas_call(
        body,
        out_shape=(
            jax.ShapeDtypeStruct((fronts, halves * cols, rows), jnp.float32),
            jax.ShapeDtypeStruct((4, 4, fronts, 16, halves * cols), jnp.bfloat16),
        ),
        in_specs=[pl.BlockSpec(memory_space=pltpu.SMEM)] + [WHOLE] * (1 + count),
        out_specs=(WHOLE, WHOLE),
        scratch_shapes=[pltpu.VMEM((fronts, rows, halves * cols), jnp.bfloat16)],
        name="finish",
    )(pos, arrived, *pieces)


def ring_pairs(cores):
    pairs = []
    for i in range(16):
        if 0 in cores:
            pairs.append((2 * i, 2 * ((i + 1) % 16)))
        if 1 in cores:
            pairs.append((2 * i + 1, 2 * ((i - 1) % 16) + 1))
    return pairs


def piece_pairs(step):
    pairs = []
    for i in range(16):
        down, up = (i - step % 8) % 16, (i + step) % 16
        pairs.append((8 * i + 2 * (i // 4), 8 * i + down // 2))
        pairs.append((8 * i + 2 * (i // 4) + 1, 8 * i + up // 2))
    return pairs


def level(boundary, owner, ancestor_cov, gain, pivot_inverse):
    w = lax.axis_index(WIDE)
    core = lax.axis_index("core")
    narrow = lax.axis_index("y") * 2 + core
    pos = jnp.stack([w, narrow, core]).astype(jnp.int32)
    swap = [(0, 1), (1, 0)]
    early = 8

    owns = [gain]
    others = [lax.ppermute(gain, "core", swap)]
    rows = gain.shape[1] // 2
    near = (w >> 1) & 1 == core
    pieces = []
    for step in range(1, 9):
        pairs = ring_pairs((0, 1) if step < 8 else (1,))
        owns.append(lax.ppermute(owns[-1], (*WIDE, "core"), pairs))
        others.append(lax.ppermute(others[-1], (*WIDE, "core"), pairs))
        a, b = owns[step], others[step]
        if step == 8:
            a = jnp.where(core == 0, owns[0], a)
            b = jnp.where(core == 0, others[0], b)
        held = jnp.where(near, a, b)
        piece = lax.dynamic_slice_in_dim(held, (w & 1) * rows, rows, 1)
        pieces.append(lax.ppermute(piece, (*WIDE, "y", "core"), piece_pairs(step)))
        if step == 1:
            arrived = lax.all_to_all(ancestor_cov, NARROW, split_axis=0, concat_axis=0, tiled=True)
            paired = lax.ppermute(arrived, "core", swap)
            left = turned(boundary, owner, pos, arrived, paired)

    mine = [products(left, owns[:early], others[:early])]
    theirs = [lax.ppermute(mine[0], "core", swap)]
    mine.append(products(left, owns[early:], others[early:]))
    theirs.append(lax.ppermute(mine[1], "core", swap))
    ready = assemble(pos, mine, theirs)
    ready = ready.reshape(4, 2, *ready.shape[1:])
    parts = lax.all_to_all(ready, "y", split_axis=0, concat_axis=0, tiled=True)

    boundary_cov, site = finish(pos, parts, pieces)
    sums = lax.all_to_all(site, "place", split_axis=0, concat_axis=0, tiled=True)
    sums = jnp.sum(sums.astype(jnp.float32), axis=0).astype(jnp.bfloat16)
    sums = lax.all_to_all(sums, "block", split_axis=0, concat_axis=0, tiled=True)
    reduced = jnp.sum(sums.astype(jnp.float32), axis=0)
    diag_cov = pivot_inverse - jnp.swapaxes(reduced, 1, 2)
    return boundary_cov, diag_cov


def solution(mesh):
    fine = Mesh(mesh.devices.reshape(4, 4, 4, 4, 2), ("front", *WIDE, "y", "core"))
    placed = (
        P("front", None),
        P(),
        P(NARROW, None, WIDE),
        P("front", NARROW, WIDE),
        P("front", NARROW, WIDE),
    )
    return jax.shard_map(
        level,
        mesh=fine,
        in_specs=placed,
        out_specs=(P("front", NARROW, WIDE), P("front", NARROW, WIDE)),
        check_vma=False,
    )
```

```python
import jax
import jax.numpy as jnp
from jax import lax
from jax.experimental import pallas as pl
from jax.experimental.pallas import tpu as pltpu
from jax.sharding import Mesh
from jax.sharding import PartitionSpec as P

BLK = 128
NARROW = ("y", "core")
WIDE = ("block", "place")
WHOLE = pl.BlockSpec(memory_space=pltpu.VMEM)


def turned(bnd, owner, pos, own, other):
    fronts, rows = bnd.shape[0], own.shape[1]
    blocks, width = bnd.shape[1] // 8, 2 * BLK

    def body(bnd_ref, owner_ref, pos_ref, own_ref, other_ref, o_ref):
        w, n = pos_ref[0], pos_ref[1]
        for m in range(fronts):
            columns = [
                pl.ds(pl.multiple_of((bnd_ref[m, 2 * w + b] - 4 * w) * BLK, BLK), BLK) for b in range(2)
            ]
            for c, (ref, at) in enumerate(((own_ref, n), (other_ref, n ^ 1))):
                for j in range(blocks):
                    source = owner_ref[bnd_ref[m, blocks * at + j]]
                    first = (c * blocks + j) * rows
                    for b in range(2):
                        block = ref[source, :, columns[b]]
                        o_ref[m, b * BLK : (b + 1) * BLK, first : first + rows] = block.T

    smem = pl.BlockSpec(memory_space=pltpu.SMEM)
    return pl.pallas_call(
        body,
        out_shape=jax.ShapeDtypeStruct((fronts, width, 2 * blocks * rows), own.dtype),
        in_specs=[smem, smem, smem, WHOLE, WHOLE],
        out_specs=WHOLE,
        name="turned",
    )(bnd, owner, pos, own, other)


def products(left, owns, others):
    fronts, rows, cols = owns[0].shape
    width = left.shape[1]
    count = len(owns)

    def body(left_ref, *refs):
        own, other, out = refs[:count], refs[count : 2 * count], refs[2 * count]
        for m in range(fronts):
            for first in range(0, count, 2):
                group = range(first, min(first + 2, count))
                near = jnp.concatenate([own[s][m] for s in group], axis=1)
                far = jnp.concatenate([other[s][m] for s in group], axis=1)
                value = jnp.dot(left_ref[m, :, :rows], near, preferred_element_type=jnp.float32)
                value += jnp.dot(left_ref[m, :, rows:], far, preferred_element_type=jnp.float32)
                for at, s in enumerate(group):
                    out[s, m] = value[:, at * cols : (at + 1) * cols].astype(jnp.bfloat16)

    flops = 4 * count * fronts * rows * cols * width
    return pl.pallas_call(
        body,
        out_shape=jax.ShapeDtypeStruct((count, fronts, width, cols), jnp.bfloat16),
        in_specs=[WHOLE] * (1 + 2 * count),
        out_specs=WHOLE,
        cost_estimate=pl.CostEstimate(
            flops=flops, transcendentals=0, bytes_accessed=4 * count * fronts * rows * cols * 2
        ),
        name="products",
    )(left, *owns, *others)


def assemble(pos, left, mine, theirs, first, second):
    count, fronts, width, cols = mine.shape
    rows = first.shape[1]

    def body(pos_ref, left_ref, mine_ref, theirs_ref, first_ref, second_ref, out):
        w, core = pos_ref[0], pos_ref[2]
        for from_core, ref in ((core, mine_ref), (1 - core, theirs_ref)):
            for step in range(count):
                to = (w + (2 * from_core - 1) * step) & 15
                wanted = ((to >> 1) & 1) == core
                if step == 0:
                    wanted = jnp.logical_and(wanted, from_core == 0)

                @pl.when(wanted)
                def _():
                    out[2 * (to >> 2) + (to & 1)] = ref[step]

        to = (w + 8) & 15

        @pl.when(((to >> 1) & 1) == core)
        def _():
            near = pl.ds(pl.multiple_of((1 - core) * rows, rows), rows)
            far = pl.ds(pl.multiple_of(core * rows, rows), rows)
            for m in range(fronts):
                value = jnp.dot(left_ref[m, :, near], first_ref[m], preferred_element_type=jnp.float32)
                value += jnp.dot(left_ref[m, :, far], second_ref[m], preferred_element_type=jnp.float32)
                out[2 * (to >> 2) + (to & 1), m] = value.astype(jnp.bfloat16)

    return pl.pallas_call(
        body,
        out_shape=jax.ShapeDtypeStruct((8, fronts, width, cols), jnp.bfloat16),
        in_specs=[pl.BlockSpec(memory_space=pltpu.SMEM)] + [WHOLE] * 5,
        out_specs=WHOLE,
        name="assemble",
    )(pos, left, mine, theirs, first, second)


def finish(pos, arrived, pieces):
    peers, halves, fronts, rows, cols = arrived.shape
    count = len(pieces)

    def body(pos_ref, a_ref, *refs):
        gs, (x_ref, d_ref, low_ref) = refs[:count], refs[count:]
        w, n = pos_ref[0], pos_ref[1]
        for m in range(fronts):
            for h in range(halves):
                total = a_ref[0, h, m].astype(jnp.float32)
                for s in range(1, peers):
                    total = total + a_ref[s, h, m].astype(jnp.float32)
                cross = -total
                x_ref[m, h * cols : (h + 1) * cols, :] = cross.T
                low_ref[m, :, h * cols : (h + 1) * cols] = cross.astype(jnp.bfloat16)
        for at, g_ref in enumerate(gs):
            step = at + 1
            down = (w - step % 8) & 15
            up = (w + step) & 15
            first = (down >> 1) == n
            half = jnp.where(first, down & 1, up & 1)

            @pl.when(jnp.logical_or(first, (up >> 1) == n))
            def _():
                for m in range(fronts):
                    site = jnp.dot(g_ref[m].T, low_ref[m], preferred_element_type=jnp.float32)
                    d_ref[pl.ds(half * 8, 8), m] = site.astype(jnp.bfloat16).reshape(8, 16, halves * cols)

    return pl.pallas_call(
        body,
        out_shape=(
            jax.ShapeDtypeStruct((fronts, halves * cols, rows), jnp.float32),
            jax.ShapeDtypeStruct((16, fronts, 16, halves * cols), jnp.bfloat16),
        ),
        in_specs=[pl.BlockSpec(memory_space=pltpu.SMEM)] + [WHOLE] * (1 + count),
        out_specs=(WHOLE, WHOLE),
        scratch_shapes=[pltpu.VMEM((fronts, rows, halves * cols), jnp.bfloat16)],
        name="finish",
    )(pos, arrived, *pieces)


def ring_pairs():
    pairs = []
    for i in range(16):
        pairs.append((2 * i, 2 * ((i + 1) % 16)))
        pairs.append((2 * i + 1, 2 * ((i - 1) % 16) + 1))
    return pairs


def last_pairs():
    return [(2 * ((i + 1) % 16) + 1, 2 * i + (i // 2) % 2) for i in range(16)]


def piece_pairs(step):
    pairs = []
    for i in range(16):
        down, up = (i - step % 8) % 16, (i + step) % 16
        upper = 1 if step < 8 else (i // 2) % 2
        pairs.append((8 * i + 2 * (i // 4) + 1 - upper, 8 * i + down // 2))
        pairs.append((8 * i + 2 * (i // 4) + upper, 8 * i + up // 2))
    return pairs


def level(boundary, owner, ancestor_cov, gain, pivot_inverse):
    w = lax.axis_index(WIDE)
    core = lax.axis_index("core")
    narrow = lax.axis_index("y") * 2 + core
    pos = jnp.stack([w, narrow, core]).astype(jnp.int32)
    swap = [(0, 1), (1, 0)]

    owns = [gain]
    others = [lax.ppermute(gain, "core", swap)]
    rows = gain.shape[1] // 2
    near = (w >> 1) & 1 == core
    pieces = []
    for step in range(1, 9):
        pairs = ring_pairs() if step < 8 else last_pairs()
        owns.append(lax.ppermute(owns[-1], (*WIDE, "core"), pairs))
        others.append(lax.ppermute(others[-1], (*WIDE, "core"), pairs))
        a, b = owns[step], others[step]
        if step < 8:
            held = jnp.where(near, a, b)
        else:
            held = jnp.where(near, jnp.where(core == 1, a, b), others[0])
        piece = lax.dynamic_slice_in_dim(held, (w & 1) * rows, rows, 1)
        pieces.append(lax.ppermute(piece, (*WIDE, "y", "core"), piece_pairs(step)))
        if step == 1:
            arrived = lax.all_to_all(
                ancestor_cov, NARROW, split_axis=0, concat_axis=0, tiled=True
            )
            paired = lax.ppermute(arrived, "core", swap)
            left = turned(boundary, owner, pos, arrived, paired)

    mine = products(left, owns[:8], others[:8])
    theirs = lax.ppermute(mine, "core", swap)
    ready = assemble(pos, left, mine, theirs, owns[8], others[8])
    ready = ready.reshape(4, 2, *ready.shape[1:])
    parts = lax.all_to_all(ready, "y", split_axis=0, concat_axis=0, tiled=True)

    boundary_cov, site = finish(pos, parts, pieces)
    sums = lax.all_to_all(site, WIDE, split_axis=0, concat_axis=0, tiled=True)
    reduced = jnp.sum(sums.astype(jnp.float32), axis=0)
    diag_cov = pivot_inverse - jnp.swapaxes(reduced, 1, 2)
    return boundary_cov, diag_cov


def solution(mesh):
    fine = Mesh(mesh.devices.reshape(4, 4, 4, 4, 2), ("front", *WIDE, "y", "core"))
    placed = (
        P("front", None),
        P(),
        P(NARROW, None, WIDE),
        P("front", NARROW, WIDE),
        P("front", NARROW, WIDE),
    )
    return jax.shard_map(
        level,
        mesh=fine,
        in_specs=placed,
        out_specs=(P("front", NARROW, WIDE), P("front", NARROW, WIDE)),
        check_vma=False,
    )
```

```python
import jax
import jax.numpy as jnp
from jax import lax
from jax.experimental import pallas as pl
from jax.experimental.pallas import tpu as pltpu
from jax.sharding import Mesh
from jax.sharding import PartitionSpec as P

BLK = 128
NARROW = ("y", "core")
WIDE = ("block", "place")
WHOLE = pl.BlockSpec(memory_space=pltpu.VMEM)


def turned(bnd, owner, pos, own, other):
    fronts, rows = bnd.shape[0], own.shape[1]
    blocks, width = bnd.shape[1] // 8, 2 * BLK

    def body(bnd_ref, owner_ref, pos_ref, own_ref, other_ref, o_ref):
        w, n = pos_ref[0], pos_ref[1]
        for m in range(fronts):
            columns = [
                pl.ds(pl.multiple_of((bnd_ref[m, 2 * w + b] - 4 * w) * BLK, BLK), BLK) for b in range(2)
            ]
            for c, (ref, at) in enumerate(((own_ref, n), (other_ref, n ^ 1))):
                for j in range(blocks):
                    source = owner_ref[bnd_ref[m, blocks * at + j]]
                    first = (c * blocks + j) * rows
                    for b in range(2):
                        block = ref[source, :, columns[b]]
                        o_ref[m, b * BLK : (b + 1) * BLK, first : first + rows] = block.T

    smem = pl.BlockSpec(memory_space=pltpu.SMEM)
    return pl.pallas_call(
        body,
        out_shape=jax.ShapeDtypeStruct((fronts, width, 2 * blocks * rows), own.dtype),
        in_specs=[smem, smem, smem, WHOLE, WHOLE],
        out_specs=WHOLE,
        name="turned",
    )(bnd, owner, pos, own, other)


def products(left, owns, others):
    fronts, rows, cols = owns[0].shape
    width = left.shape[1]
    count = len(owns)

    def body(left_ref, *refs):
        own, other, out = refs[:count], refs[count : 2 * count], refs[2 * count]
        for first in range(0, count, 2):
            group = range(first, min(first + 2, count))
            near = jnp.concatenate([own[s][...] for s in group], axis=1)
            far = jnp.concatenate([other[s][...] for s in group], axis=1)
            value = jnp.dot(left_ref[:, :rows], near, preferred_element_type=jnp.float32)
            value += jnp.dot(left_ref[:, rows:], far, preferred_element_type=jnp.float32)
            for at, s in enumerate(group):
                out[s] = value[:, at * cols : (at + 1) * cols].astype(jnp.bfloat16)

    flops = 4 * count * fronts * rows * cols * width
    chunk = pl.BlockSpec((None, rows, cols), lambda m: (m, 0, 0))
    return pl.pallas_call(
        body,
        grid=(fronts,),
        out_shape=jax.ShapeDtypeStruct((count, fronts, width, cols), jnp.bfloat16),
        in_specs=[pl.BlockSpec((None, width, 2 * rows), lambda m: (m, 0, 0))] + [chunk] * (2 * count),
        out_specs=pl.BlockSpec((count, None, width, cols), lambda m: (0, m, 0, 0)),
        cost_estimate=pl.CostEstimate(
            flops=flops, transcendentals=0, bytes_accessed=4 * count * fronts * rows * cols * 2
        ),
        name="products",
    )(left, *owns, *others)


def assemble(pos, left, mine, theirs, first, second):
    count, fronts, width, cols = mine.shape
    rows = first.shape[1]

    def body(pos_ref, left_ref, mine_ref, theirs_ref, first_ref, second_ref, out):
        w, core = pos_ref[0], pos_ref[2]
        for from_core, ref in ((core, mine_ref), (1 - core, theirs_ref)):
            for step in range(count):
                to = (w + (2 * from_core - 1) * step) & 15
                wanted = ((to >> 1) & 1) == core
                if step == 0:
                    wanted = jnp.logical_and(wanted, from_core == 0)

                @pl.when(wanted)
                def _():
                    out[2 * (to >> 2) + (to & 1)] = ref[step]

        to = (w + 8) & 15

        @pl.when(((to >> 1) & 1) == core)
        def _():
            near = pl.ds(pl.multiple_of((1 - core) * rows, rows), rows)
            far = pl.ds(pl.multiple_of(core * rows, rows), rows)
            value = jnp.dot(left_ref[:, near], first_ref[...], preferred_element_type=jnp.float32)
            value += jnp.dot(left_ref[:, far], second_ref[...], preferred_element_type=jnp.float32)
            out[2 * (to >> 2) + (to & 1)] = value.astype(jnp.bfloat16)

    parts = pl.BlockSpec((count, None, width, cols), lambda m: (0, m, 0, 0))
    chunk = pl.BlockSpec((None, rows, cols), lambda m: (m, 0, 0))
    return pl.pallas_call(
        body,
        grid=(fronts,),
        out_shape=jax.ShapeDtypeStruct((8, fronts, width, cols), jnp.bfloat16),
        in_specs=[
            pl.BlockSpec(memory_space=pltpu.SMEM),
            pl.BlockSpec((None, width, 2 * rows), lambda m: (m, 0, 0)),
            parts,
            parts,
            chunk,
            chunk,
        ],
        out_specs=pl.BlockSpec((8, None, width, cols), lambda m: (0, m, 0, 0)),
        name="assemble",
    )(pos, left, mine, theirs, first, second)


def total(arrived):
    peers, halves, fronts, rows, cols = arrived.shape

    def body(a_ref, x_ref, low_ref):
        for h in range(halves):
            value = a_ref[0, h].astype(jnp.float32)
            for s in range(1, peers):
                value = value + a_ref[s, h].astype(jnp.float32)
            cross = -value
            x_ref[h * cols : (h + 1) * cols, :] = cross.T
            low_ref[:, h * cols : (h + 1) * cols] = cross.astype(jnp.bfloat16)

    return pl.pallas_call(
        body,
        grid=(fronts,),
        out_shape=(
            jax.ShapeDtypeStruct((fronts, halves * cols, rows), jnp.float32),
            jax.ShapeDtypeStruct((fronts, rows, halves * cols), jnp.bfloat16),
        ),
        in_specs=[pl.BlockSpec((peers, halves, None, rows, cols), lambda m: (0, 0, m, 0, 0))],
        out_specs=(
            pl.BlockSpec((None, halves * cols, rows), lambda m: (m, 0, 0)),
            pl.BlockSpec((None, rows, halves * cols), lambda m: (m, 0, 0)),
        ),
        name="total",
    )(arrived)


def sites(pos, low, pieces):
    fronts, rows, pivots = low.shape
    count = len(pieces)

    def body(pos_ref, low_ref, *refs):
        gs, d_ref = refs[:count], refs[count]
        w, n = pos_ref[0], pos_ref[1]
        for at, g_ref in enumerate(gs):
            step = at + 1
            down = (w - step % 8) & 15
            up = (w + step) & 15
            first = (down >> 1) == n
            half = jnp.where(first, down & 1, up & 1)

            @pl.when(jnp.logical_or(first, (up >> 1) == n))
            def _():
                site = jnp.dot(g_ref[...].T, low_ref[...], preferred_element_type=jnp.float32)
                d_ref[pl.ds(half * 8, 8)] = site.astype(jnp.bfloat16).reshape(8, 16, pivots)

    piece = pl.BlockSpec((None, rows, BLK), lambda m: (m, 0, 0))
    return pl.pallas_call(
        body,
        grid=(fronts,),
        out_shape=jax.ShapeDtypeStruct((16, fronts, 16, pivots), jnp.bfloat16),
        in_specs=[
            pl.BlockSpec(memory_space=pltpu.SMEM),
            pl.BlockSpec((None, rows, pivots), lambda m: (m, 0, 0)),
        ]
        + [piece] * count,
        out_specs=pl.BlockSpec((16, None, 16, pivots), lambda m: (0, m, 0, 0)),
        name="sites",
    )(pos, low, *pieces)


def ring_pairs():
    pairs = []
    for i in range(16):
        pairs.append((2 * i, 2 * ((i + 1) % 16)))
        pairs.append((2 * i + 1, 2 * ((i - 1) % 16) + 1))
    return pairs


def last_pairs():
    return [(2 * ((i + 1) % 16) + 1, 2 * i + (i // 2) % 2) for i in range(16)]


def piece_pairs(step):
    pairs = []
    for i in range(16):
        down, up = (i - step % 8) % 16, (i + step) % 16
        upper = 1 if step < 8 else (i // 2) % 2
        pairs.append((8 * i + 2 * (i // 4) + 1 - upper, 8 * i + down // 2))
        pairs.append((8 * i + 2 * (i // 4) + upper, 8 * i + up // 2))
    return pairs


def level(boundary, owner, ancestor_cov, gain, pivot_inverse):
    w = lax.axis_index(WIDE)
    core = lax.axis_index("core")
    narrow = lax.axis_index("y") * 2 + core
    pos = jnp.stack([w, narrow, core]).astype(jnp.int32)
    swap = [(0, 1), (1, 0)]

    owns = [gain]
    others = [lax.ppermute(gain, "core", swap)]
    rows = gain.shape[1] // 2
    near = (w >> 1) & 1 == core
    pieces = []
    for step in range(1, 9):
        pairs = ring_pairs() if step < 8 else last_pairs()
        owns.append(lax.ppermute(owns[-1], (*WIDE, "core"), pairs))
        others.append(lax.ppermute(others[-1], (*WIDE, "core"), pairs))
        a, b = owns[step], others[step]
        if step < 8:
            held = jnp.where(near, a, b)
        else:
            held = jnp.where(near, jnp.where(core == 1, a, b), others[0])
        piece = lax.dynamic_slice_in_dim(held, (w & 1) * rows, rows, 1)
        pieces.append(lax.ppermute(piece, (*WIDE, "y", "core"), piece_pairs(step)))
        if step == 1:
            arrived = lax.all_to_all(ancestor_cov, NARROW, split_axis=0, concat_axis=0, tiled=True)
            paired = lax.ppermute(arrived, "core", swap)
            left = turned(boundary, owner, pos, arrived, paired)

    mine = products(left, owns[:8], others[:8])
    theirs = lax.ppermute(mine, "core", swap)
    ready = assemble(pos, left, mine, theirs, owns[8], others[8])
    ready = ready.reshape(4, 2, *ready.shape[1:])
    parts = lax.all_to_all(ready, "y", split_axis=0, concat_axis=0, tiled=True)

    boundary_cov, low = total(parts)
    site = sites(pos, low, pieces)
    sums = lax.all_to_all(site, WIDE, split_axis=0, concat_axis=0, tiled=True)
    reduced = jnp.sum(sums.astype(jnp.float32), axis=0)
    diag_cov = pivot_inverse - jnp.swapaxes(reduced, 1, 2)
    return boundary_cov, diag_cov


def solution(mesh):
    fine = Mesh(mesh.devices.reshape(4, 4, 4, 4, 2), ("front", *WIDE, "y", "core"))
    placed = (
        P("front", None),
        P(),
        P(NARROW, None, WIDE),
        P("front", NARROW, WIDE),
        P("front", NARROW, WIDE),
    )
    return jax.shard_map(
        level,
        mesh=fine,
        in_specs=placed,
        out_specs=(P("front", NARROW, WIDE), P("front", NARROW, WIDE)),
        check_vma=False,
    )
```
